32 devices in a mesh: cp: 8 (over z, x), tp: 4 (over y, core).
Axes of the slice: x: 2, y: 2, z: 4, core: 2. Of those that a mesh axis runs over, the one named last changes fastest.
Arguments:
- queries: bfloat16 [1536, 2048], P('cp', 'tp'), may hold values from -128 to 128
- keys: bfloat16 [1536, 256], P('cp'), may hold values from -6 to 6
- values: bfloat16 [1536, 256], P('cp'), may hold values from -6 to 6
- positions: int32 [1536], replicated, may hold values from 0 to 1535, as said below
- out_weight: bfloat16 [2048, 8192], P('tp'), may hold values from -0.125 to 0.125
Outputs:
- mixed: bfloat16 [1536, 8192], P(('cp', 'tp'))
The draws below stay inside these ranges and needn't reach their ends.
Inputs may be any that keep to these rules, and one draw needn't show every extreme that they name: positions is a permutation of 0 to 1535. The tokens stored at indices d * 192 to (d + 1) * 192 - 1 form two runs of 96 consecutive positions, the first starting at b * 96 and the second at (15 - b) * 96 for some b, each b used by one d.
All inputs are finite; a program needn't handle non-finite values.
Results may differ from the reference program's by a relative error of at most 0.013.
Values may be sent and summed in bfloat16 or wider, within the bound.
A program may use at most 128 MiB of HBM per device.

```python
import math
import jax
import jax.numpy as jnp
from jax import lax

D = 8192
HEAD = 128
GROUP = 8
KV = 2
TOK_DEV = 192
H = 16
TOKENS = 1536
N_TP = 4


def joint_draw(key):
    seed_base = jax.random.fold_in(key, 11)
    seed_query, seed_keys = jax.random.split(seed_base, 2)
    queries = jnp.clip(jax.random.normal(seed_query, (TOKENS, GROUP * KV * HEAD), jnp.float32), -6.0, 6.0)
    keys = jnp.clip(jax.random.normal(seed_keys, (TOKENS, KV * HEAD), jnp.float32), -6.0, 6.0)
    return (queries, keys)


def draw_queries(key, part):
    return joint_draw(key)[0].astype(jnp.bfloat16)


def draw_keys(key, part):
    return joint_draw(key)[1].astype(jnp.bfloat16)


def draw_positions(key, part):
    slot_count = TOKENS // TOK_DEV
    half_rows = TOK_DEV // 2
    slot_order = jax.random.permutation(jax.random.fold_in(key, 5), slot_count)
    block_start = jnp.stack([slot_order, 2 * slot_count - 1 - slot_order], axis=1)
    position = block_start[:, :, None] * half_rows + jnp.arange(half_rows)[None, None, :]
    return position.reshape(-1).astype(jnp.int32)


def block_levels(own_key, extent, shards, smallest, top_value):
    gain, own = 1.0, jax.random.fold_in(own_key, 6)
    for axis_at, parts in shards:
        heights = jnp.exp(jax.random.uniform(jax.random.fold_in(own, axis_at), (parts,), jnp.float32, smallest / len(shards), top_value / len(shards)))
        gain = gain * jnp.repeat(heights, extent[axis_at] // parts).reshape([-1 if axis == axis_at else 1 for axis in range(len(extent))])
    return gain


def bell_draw(own_key, extent, spread, most, cuts=(), kind=jnp.bfloat16):
    level = block_levels(own_key, extent, cuts, -0.22, 0.18) if cuts else 1.0
    entries = jax.random.normal(own_key, extent, jnp.float32) * spread * level
    return jnp.minimum(jnp.maximum(entries, -most), most).astype(kind)


def setup_inputs(seed: int = 0) -> dict:
    splits = jax.random.split(jax.random.key(seed), 6)
    queries = draw_queries(jax.random.fold_in(splits[5], 71), 0)
    keys = draw_keys(jax.random.fold_in(splits[5], 71), 0)
    values = bell_draw(splits[2], (TOKENS, KV * HEAD), 1.0, 6.0, ((0, 8),))
    positions = draw_positions(jax.random.fold_in(splits[5], 71), 0)
    out_weight = bell_draw(splits[4], (H * HEAD, D), (H * HEAD) ** -0.5, 0.125, ((0, 4),))
    return dict(queries=queries, keys=keys, values=values, positions=positions, out_weight=out_weight)


def reference(queries, keys, values, positions, out_weight):
    token_count = queries.shape[0]
    head_count = queries.shape[1] // HEAD
    score_scale = HEAD ** -0.5
    block_rows = math.gcd(token_count, 512)

    def one_block(block_index):
        first = (block_index * block_rows).astype(jnp.int32)
        query_block = lax.dynamic_slice_in_dim(queries, first, block_rows, 0)
        query_pos = lax.dynamic_slice_in_dim(positions, first, block_rows, 0)
        allowed = positions[None, :] <= query_pos[:, None]

        def one_head(head_index):
            kv_group = head_index // GROUP
            query_head = lax.dynamic_slice_in_dim(query_block, (head_index * HEAD).astype(jnp.int32), HEAD, 1)
            key_head = lax.dynamic_slice_in_dim(keys, (kv_group * HEAD).astype(jnp.int32), HEAD, 1)
            value_head = lax.dynamic_slice_in_dim(values, (kv_group * HEAD).astype(jnp.int32), HEAD, 1)
            scores = jnp.dot(query_head, key_head.T, preferred_element_type=jnp.float32) * score_scale
            scores = jnp.where(allowed, scores, -1e30)
            row_max = jnp.max(scores, axis=1, keepdims=True)
            weights = jnp.where(allowed, jnp.exp(scores - row_max), 0.0)
            row_sum = jnp.sum(weights, axis=1, keepdims=True)
            head_out = jnp.dot(weights.astype(jnp.bfloat16), value_head, preferred_element_type=jnp.float32) / row_sum
            return head_out.astype(jnp.bfloat16)

        stacked = lax.map(one_head, jnp.arange(head_count, dtype=jnp.int32))
        return jnp.transpose(stacked, (1, 0, 2)).reshape(block_rows, head_count * HEAD)

    attended = lax.map(one_block, jnp.arange(token_count // block_rows, dtype=jnp.int32))
    attended = attended.reshape(token_count, head_count * HEAD)
    slab_width = attended.shape[1] // N_TP
    mixed = jnp.zeros((token_count, out_weight.shape[1]), jnp.float32)
    for slab in range(N_TP):
        partial_sum = jnp.dot(attended[:, slab * slab_width:(slab + 1) * slab_width],
                              out_weight[slab * slab_width:(slab + 1) * slab_width],
                              preferred_element_type=jnp.float32).astype(jnp.bfloat16)
        partial_sum = lax.optimization_barrier(partial_sum)
        mixed = mixed + partial_sum.astype(jnp.float32)
    return mixed.astype(jnp.bfloat16)
```

```python
import functools
import math

import jax
import jax.numpy as jnp
from jax import lax
from jax.experimental import pallas as pl
from jax.experimental.pallas import tpu as pltpu
from jax.sharding import PartitionSpec as P

HEAD = 128
GROUP = 8
CORES = 2
PAIR = 2
CHUNK = 512
W_PARTS = 4
LOG2E = math.log2(math.e)
NT = (((1,), (1,)), ((), ()))


def kernel(
    groups,
    pos,
    q,
    k,
    v,
    w,
    got,
    mine,
    qs,
    kv,
    wb,
    att,
    top,
    total,
    acc,
    far,
    near,
    load_sem,
    wl_sem,
    d_send,
    d_recv,
    x_send,
    x_recv,
    c_send,
    c_recv,
    w_send,
    w_recv,
    a_send,
    a_recv,
    y_send,
    y_recv,
    m_send,
    m_recv,
    m_local,
):
    tok = q.shape[0]
    heads = q.shape[1] // HEAD
    run = tok // 2
    part = run // CORES
    half_cols = w.shape[1] // CORES
    chunks = half_cols // CHUNK
    rows = heads * run
    span = PAIR * tok

    cp = lax.axis_index("cp")
    tp = lax.axis_index("tp")
    y = tp // CORES
    core = lax.rem(tp, CORES)
    mate = 1 - core
    far_y = 1 - y
    z = cp // PAIR
    side = lax.rem(cp, PAIR)
    kv_group = tp * heads // GROUP

    def dev(c, t):
        return {"cp": c, "tp": t}

    x_dev = dev(z * PAIR + 1 - side, tp)
    mate_dev = dev(cp, y * CORES + mate)

    def remote(src, dst, ssem, rsem, to):
        return pltpu.make_async_remote_copy(
            src_ref=src,
            dst_ref=dst,
            send_sem=ssem,
            recv_sem=rsem,
            device_id=to,
            device_id_type=pl.DeviceIdType.MESH,
        )

    def block(kind, zz, ss):
        return kv.at[kind, zz, pl.ds(pl.multiple_of(ss * tok, tok), tok)]

    cols = pl.ds(pl.multiple_of(kv_group * HEAD, HEAD), HEAD)
    loads = [
        pltpu.make_async_copy(k.at[:, cols], block(0, z, side), load_sem.at[0]),
        pltpu.make_async_copy(v.at[:, cols], block(1, z, side), load_sem.at[1]),
    ]
    q_loads = []
    for s, yy in ((0, far_y), (1, y)):
        for h in range(heads):
            q_loads.append(
                pltpu.make_async_copy(
                    q.at[pl.ds(pl.multiple_of(yy * run, run), run), pl.ds(h * HEAD, HEAD)],
                    qs.at[s, pl.ds(h * run, run)],
                    load_sem.at[2 + s * heads + h],
                )
            )
    piece = half_cols // W_PARTS
    w_loads, w_sends = [], []
    for i in range(W_PARTS):
        own = pl.ds(pl.multiple_of(core * half_cols + i * piece, piece), piece)
        other = pl.ds(pl.multiple_of(mate * half_cols + i * piece, piece), piece)
        here = pl.ds(i * piece, piece)
        w_loads.append(pltpu.make_async_copy(w.at[:, own], wb.at[0, :, here], wl_sem.at[i]))
        w_sends.append(
            remote(w.at[:, other], wb.at[1, :, here], w_send.at[i], w_recv.at[i], mate_dev)
        )
    for c in loads + q_loads:
        c.start()

    barrier = pltpu.get_barrier_semaphore()
    peers = [dev(lax.rem(z + off, groups) * PAIR + side, tp) for off in range(1, groups)]
    y_devs = [dev(cp, far_y * CORES + c) for c in range(CORES)]
    greet = peers + [x_dev, mate_dev] + y_devs
    for d in greet:
        pl.semaphore_signal(barrier, inc=1, device_id=d, device_id_type=pl.DeviceIdType.MESH)
    pl.semaphore_wait(barrier, len(greet))

    for c in loads:
        c.wait()
    own = block(core, z, side)
    sent = []
    x_own = remote(own, own, x_send.at[z], x_recv.at[z], x_dev)
    x_own.start()
    sent.append(x_own)
    for i, d in enumerate(peers):
        c = remote(own, own, d_send.at[i], d_recv.at[z], d)
        c.start()
        sent.append(c)
    for c in w_sends:
        c.start()
        sent.append(c)
    for c in w_loads:
        c.start()

    def hand(kind, zz, ss):
        b = block(kind, zz, ss)
        c = remote(b, b, c_send.at[zz, ss], c_recv.at[zz, ss], mate_dev)
        c.start()
        sent.append(c)

    def arrived_x(zz):
        b = block(core, zz, 1 - side)
        remote(b, b, x_send.at[zz], x_recv.at[zz], x_dev).wait_recv()
        hand(core, zz, 1 - side)

    def arrived_d(zz):
        b = block(core, zz, side)
        remote(b, b, d_send.at[0], d_recv.at[zz], x_dev).wait_recv()
        c = remote(b, b, x_send.at[zz], x_recv.at[zz], x_dev)
        c.start()
        sent.append(c)
        hand(core, zz, side)

    def arrived_c(zz, ss):
        b = block(mate, zz, ss)
        remote(b, b, c_send.at[zz, ss], c_recv.at[zz, ss], mate_dev).wait_recv()

    def attend(zz, s, first):
        yy = far_y if s == 0 else y
        keys = kv[0, zz]
        vals = kv[1, zz]
        scores = lax.dot_general(qs[s], keys, NT, preferred_element_type=jnp.float32)
        j = lax.broadcasted_iota(jnp.int32, (1, span), 1)
        base = zz * span
        key_pos = j + pos[base]
        for i in range(1, span // run):
            key_pos = jnp.where(j >= i * run, j + (pos[base + i * run] - i * run), key_pos)
        i = lax.rem(lax.broadcasted_iota(jnp.int32, (rows, 1), 0), run)
        query_pos = i + pos[cp * tok + yy * run]
        scores = jnp.where(key_pos <= query_pos, scores, -1e30)
        peak = jnp.max(scores, axis=1, keepdims=True)
        if not first:
            old = top[s]
            peak = jnp.maximum(old, peak)
        factor = HEAD**-0.5 * LOG2E
        weights = jnp.exp2((scores - peak) * factor)
        part_sum = jnp.sum(weights, axis=1, keepdims=True)
        part_out = jnp.dot(
            weights.astype(jnp.bfloat16), vals, preferred_element_type=jnp.float32
        )
        if not first:
            fade = jnp.exp2((old - peak) * factor)
            part_sum = total[s] * fade + part_sum
            part_out = acc[s] * fade + part_out
        top[s] = peak
        total[s] = part_sum
        acc[s] = part_out

    order = [lax.rem(z + groups - off, groups) for off in range(1, groups)]
    arrived_x(z)
    small = groups <= 4
    for c in q_loads:
        c.wait()

    def finish(s):
        out = (acc[s] / total[s]).astype(jnp.bfloat16)
        for h in range(heads):
            att[0, s, :, h * HEAD : (h + 1) * HEAD] = out[h * run : (h + 1) * run]
        c = remote(att.at[0, s], att.at[1, s], a_send.at[s], a_recv.at[s], mate_dev)
        c.start()
        sent.append(c)
        return c

    def own_group():
        arrived_c(z, 1 - side)
        attend(z, 0, True)
        attend(z, 1, True)

    if small:
        for zz in order[:-1]:
            arrived_d(zz)
        own_group()
        arrived_d(order[-1])
        for zz in order[:-1]:
            arrived_x(zz)
        for zz in order[:-2]:
            arrived_c(zz, side)
            arrived_c(zz, 1 - side)
            attend(zz, 0, False)
            attend(zz, 1, False)
        arrived_x(order[-1])
        for s in range(2):
            for zz in order[-2:]:
                if s == 0:
                    arrived_c(zz, side)
                    arrived_c(zz, 1 - side)
                attend(zz, s, False)
            if s == 0:
                swap_0 = finish(0)
        swap_1 = finish(1)
    else:
        for zz in order:
            arrived_d(zz)
        for zz in order:
            arrived_x(zz)
        own_group()

        def step(off, carry):
            zz = lax.rem(z + groups - off, groups)
            arrived_c(zz, side)
            arrived_c(zz, 1 - side)
            attend(zz, 0, False)
            attend(zz, 1, False)
            return carry

        lax.fori_loop(1, groups, step, 0)
        swap_0 = finish(0)
        swap_1 = finish(1)

    for c in w_loads:
        c.wait()
    for c in w_sends:
        c.wait_recv()

    def project(s, n):
        at = pl.ds(n * CHUNK, CHUNK)
        return (
            jnp.dot(att[0, s], wb[0, :, at], preferred_element_type=jnp.float32)
            + jnp.dot(att[1, s], wb[1, :, at], preferred_element_type=jnp.float32)
        ).astype(jnp.bfloat16)

    def place(ref, c, n):
        return ref.at[:, pl.ds(pl.multiple_of(c * half_cols + n * CHUNK, CHUNK), CHUNK)]

    swap_0.wait_recv()
    far_in = []
    for n in range(chunks):
        out = project(0, n)
        for c in range(CORES):
            far[n, c] = out[c * part : (c + 1) * part]
        for c in range(CORES):
            cc = remote(
                far.at[n, c], place(got, core, n), y_send.at[n, c], y_recv.at[n, core], y_devs[c]
            )
            cc.start()
            sent.append(cc)
            far_in.append((n, c))
    swap_1.wait_recv()
    local_copies, near_sends = [], []
    for n in range(chunks):
        out = project(1, n)
        for c in range(CORES):
            near[n, c] = out[c * part : (c + 1) * part]
        lc = pltpu.make_async_copy(near.at[n, core], place(mine, core, n), m_local.at[n])
        lc.start()
        local_copies.append(lc)
        rc = remote(near.at[n, mate], place(mine, core, n), m_send.at[n], m_recv.at[n], mate_dev)
        rc.start()
        near_sends.append(rc)

    for c in local_copies:
        c.wait()
    for n, c in enumerate(near_sends):
        c.wait_send()
        remote(
            near.at[n, mate], place(mine, mate, n), m_send.at[n], m_recv.at[n], mate_dev
        ).wait_recv()
    for c in sent:
        c.wait_send()
    for n, c in far_in:
        remote(
            far.at[n, c], place(got, c, n), y_send.at[n, c], y_recv.at[n, c], y_devs[c]
        ).wait_recv()


def shards(groups, queries, keys, values, positions, out_weight):
    tok, width = queries.shape
    heads = width // HEAD
    run = tok // 2
    part = run // CORES
    depth, cols = out_weight.shape
    half_cols = cols // CORES
    chunks = half_cols // CHUNK
    rows = heads * run
    dma = pltpu.SemaphoreType.DMA
    out = jax.ShapeDtypeStruct((part, cols), jnp.bfloat16)
    any_spec = pl.BlockSpec(memory_space=pl.ANY)
    got, mine = pl.pallas_call(
        functools.partial(kernel, groups),
        out_shape=(out, out),
        in_specs=[pl.BlockSpec(memory_space=pltpu.SMEM)] + [any_spec] * 4,
        out_specs=(any_spec, any_spec),
        scratch_shapes=[
            pltpu.VMEM((2, rows, HEAD), jnp.bfloat16),
            pltpu.VMEM((2, groups, PAIR * tok, HEAD), jnp.bfloat16),
            pltpu.VMEM((2, depth, half_cols), jnp.bfloat16),
            pltpu.VMEM((2, 2, run, width), jnp.bfloat16),
            pltpu.VMEM((2, rows, 1), jnp.float32),
            pltpu.VMEM((2, rows, 1), jnp.float32),
            pltpu.VMEM((2, rows, HEAD), jnp.float32),
            pltpu.VMEM((chunks, CORES, part, CHUNK), jnp.bfloat16),
            pltpu.VMEM((chunks, CORES, part, CHUNK), jnp.bfloat16),
            dma((2 + 2 * heads,)),
            dma((W_PARTS,)),
            dma((groups,)),
            dma((groups,)),
            dma((groups,)),
            dma((groups,)),
            dma((groups, PAIR)),
            dma((groups, PAIR)),
            dma((W_PARTS,)),
            dma((W_PARTS,)),
            dma((2,)),
            dma((2,)),
            dma((chunks, CORES)),
            dma((chunks, CORES)),
            dma((chunks,)),
            dma((chunks,)),
            dma((chunks,)),
        ],
        compiler_params=pltpu.CompilerParams(collective_id=0, has_side_effects=True),
    )(positions, queries, keys, values, out_weight)
    return (got.astype(jnp.float32) + mine.astype(jnp.float32)).astype(jnp.bfloat16)


def solution(mesh):
    groups = mesh.shape["cp"] // PAIR
    in_specs = (P("cp", "tp"), P("cp", None), P("cp", None), P(), P("tp", None))
    out_specs = P(("cp", "tp"), None)
    return jax.shard_map(
        functools.partial(shards, groups),
        mesh=mesh,
        in_specs=in_specs,
        out_specs=out_specs,
        check_vma=False,
    )
```

```python
import functools
import math

import jax
import jax.numpy as jnp
from jax import lax
from jax.experimental import pallas as pl
from jax.experimental.pallas import tpu as pltpu
from jax.sharding import PartitionSpec as P

HEAD = 128
GROUP = 8
CORES = 2
PAIR = 2
CHUNK = 512
W_PARTS = 8
PIECES = 2
LOG2E = math.log2(math.e)
NT = (((1,), (1,)), ((), ()))


def kernel(
    groups,
    pos,
    q,
    k,
    v,
    w,
    got,
    mine,
    qs,
    kv,
    wb,
    att,
    top,
    total,
    acc,
    far,
    near,
    load_sem,
    wl_sem,
    d_send,
    o_send,
    d_recv,
    x_send,
    x_recv,
    c_send,
    c_recv,
    w_send,
    w_recv,
    a_send,
    a_recv,
    y_send,
    y_recv,
    m_send,
    m_recv,
    m_local,
):
    tok = q.shape[0]
    heads = q.shape[1] // HEAD
    run = tok // 2
    part = run // CORES
    half_cols = w.shape[1] // CORES
    chunks = half_cols // CHUNK
    rows = heads * run
    span = PAIR * tok

    cp = lax.axis_index("cp")
    tp = lax.axis_index("tp")
    y = tp // CORES
    core = lax.rem(tp, CORES)
    mate = 1 - core
    far_y = 1 - y
    z = cp // PAIR
    side = lax.rem(cp, PAIR)
    kv_group = tp * heads // GROUP

    def dev(c, t):
        return {"cp": c, "tp": t}

    x_dev = dev(z * PAIR + 1 - side, tp)
    mate_dev = dev(cp, y * CORES + mate)

    def remote(src, dst, ssem, rsem, to):
        return pltpu.make_async_remote_copy(
            src_ref=src,
            dst_ref=dst,
            send_sem=ssem,
            recv_sem=rsem,
            device_id=to,
            device_id_type=pl.DeviceIdType.MESH,
        )

    def block(kind, zz, ss, at=None):
        if at is None:
            return kv.at[kind, zz, pl.ds(pl.multiple_of(ss * tok, tok), tok)]
        size = tok // PIECES
        return kv.at[kind, zz, pl.ds(pl.multiple_of(ss * tok + at * size, size), size)]

    cols = pl.ds(pl.multiple_of(kv_group * HEAD, HEAD), HEAD)
    loads = [
        pltpu.make_async_copy(k.at[:, cols], block(0, z, side), load_sem.at[0]),
        pltpu.make_async_copy(v.at[:, cols], block(1, z, side), load_sem.at[1]),
    ]
    q_loads = []
    for s, yy in ((0, far_y), (1, y)):
        for h in range(heads):
            q_loads.append(
                pltpu.make_async_copy(
                    q.at[pl.ds(pl.multiple_of(yy * run, run), run), pl.ds(h * HEAD, HEAD)],
                    qs.at[s, pl.ds(h * run, run)],
                    load_sem.at[2 + s * heads + h],
                )
            )
    piece = half_cols // W_PARTS
    w_loads, w_sends = [], []
    for i in range(W_PARTS):
        own = pl.ds(pl.multiple_of(core * half_cols + i * piece, piece), piece)
        other = pl.ds(pl.multiple_of(mate * half_cols + i * piece, piece), piece)
        here = pl.ds(i * piece, piece)
        w_loads.append(pltpu.make_async_copy(w.at[:, own], wb.at[0, :, here], wl_sem.at[i]))
        w_sends.append(
            remote(w.at[:, other], wb.at[1, :, here], w_send.at[i], w_recv.at[i], mate_dev)
        )
    for c in loads + q_loads:
        c.start()

    barrier = pltpu.get_barrier_semaphore()
    y_devs = [dev(cp, far_y * CORES + c) for c in range(CORES)]
    has_left = z > 0
    has_right = z < groups - 1
    left = dev(jnp.maximum(z - 1, 0) * PAIR + side, tp)
    right = dev(jnp.minimum(z + 1, groups - 1) * PAIR + side, tp)

    def greet(d):
        pl.semaphore_signal(barrier, inc=1, device_id=d, device_id_type=pl.DeviceIdType.MESH)

    always = [x_dev, mate_dev] + y_devs
    for d in always:
        greet(d)
    pl.when(has_left)(lambda: greet(left))
    pl.when(has_right)(lambda: greet(right))
    sides = jnp.where(has_left, 1, 0) + jnp.where(has_right, 1, 0)
    pl.semaphore_wait(barrier, len(always) + sides)

    for c in loads:
        c.wait()
    sent = []
    sent_if = []

    def start(c, when=None):
        if when is None:
            c.start()
            sent.append(c)
        else:
            pl.when(when)(c.start)
            sent_if.append((when, c))

    for p in range(PIECES):
        own = block(core, z, side, p)
        start(remote(own, own, d_send.at[z, p], d_recv.at[z, p], left), has_left)
        start(remote(own, own, o_send.at[p], d_recv.at[z, p], right), has_right)
        start(remote(own, own, x_send.at[z, p], x_recv.at[z, p], x_dev))
    waiting = list(w_sends)

    def swap_w(count):
        for c in waiting[:count]:
            start(c)
        del waiting[:count]

    swap_w(3)
    for c in w_loads:
        c.start()

    near_z = jnp.minimum(z, groups - 1 - z)
    long_side = jnp.where(2 * z < groups, 1, -1)

    def arrival(i):
        turn = jnp.where(lax.rem(i, 2) == 1, -((i + 1) // 2), i // 2)
        return z + jnp.where(i <= 2 * near_z, turn, long_side * (i - near_z))

    def hand(zz, ss, p):
        b = block(core, zz, ss, p)
        start(remote(b, b, c_send.at[zz, ss, p], c_recv.at[zz, ss, p], mate_dev))

    def arrived_x(zz):
        for p in range(PIECES):
            b = block(core, zz, 1 - side, p)
            remote(b, b, x_send.at[zz, p], x_recv.at[zz, p], x_dev).wait_recv()
            hand(zz, 1 - side, p)

    def arrived_d(zz):
        onward = jnp.where(zz < z, z + 1, z - 1)
        inside = (onward >= 0) & (onward < groups)
        to = dev(jnp.clip(onward, 0, groups - 1) * PAIR + side, tp)
        for p in range(PIECES):
            b = block(core, zz, side, p)
            remote(b, b, d_send.at[zz, p], d_recv.at[zz, p], x_dev).wait_recv()
            start(remote(b, b, d_send.at[zz, p], d_recv.at[zz, p], to), inside)
            start(remote(b, b, x_send.at[zz, p], x_recv.at[zz, p], x_dev))
            hand(zz, side, p)

    def arrived_c(zz, ss):
        for p in range(PIECES):
            b = block(mate, zz, ss, p)
            remote(b, b, c_send.at[zz, ss, p], c_recv.at[zz, ss, p], mate_dev).wait_recv()

    def attend(zz, s, first):
        yy = far_y if s == 0 else y
        keys = kv[0, zz]
        vals = kv[1, zz]
        scores = lax.dot_general(qs[s], keys, NT, preferred_element_type=jnp.float32)
        j = lax.broadcasted_iota(jnp.int32, (1, span), 1)
        base = zz * span
        key_pos = j + pos[base]
        for i in range(1, span // run):
            key_pos = jnp.where(j >= i * run, j + (pos[base + i * run] - i * run), key_pos)
        i = lax.rem(lax.broadcasted_iota(jnp.int32, (rows, 1), 0), run)
        query_pos = i + pos[cp * tok + yy * run]
        scores = jnp.where(key_pos <= query_pos, scores, -1e30)
        peak = jnp.max(scores, axis=1, keepdims=True)
        if not first:
            old = top[s]
            peak = jnp.maximum(old, peak)
        factor = HEAD**-0.5 * LOG2E
        weights = jnp.exp2((scores - peak) * factor)
        part_sum = jnp.sum(weights, axis=1, keepdims=True)
        part_out = jnp.dot(
            weights.astype(jnp.bfloat16), vals, preferred_element_type=jnp.float32
        )
        if not first:
            fade = jnp.exp2((old - peak) * factor)
            part_sum = total[s] * fade + part_sum
            part_out = acc[s] * fade + part_out
        top[s] = peak
        total[s] = part_sum
        acc[s] = part_out

    arrived_x(z)
    swap_w(1)

    def finish(s):
        out = (acc[s] / total[s]).astype(jnp.bfloat16)
        for h in range(heads):
            att[0, s, :, h * HEAD : (h + 1) * HEAD] = out[h * run : (h + 1) * run]
        c = remote(att.at[0, s], att.at[1, s], a_send.at[s], a_recv.at[s], mate_dev)
        c.start()
        sent.append(c)
        return c

    def arrived_group(zz):
        arrived_c(zz, side)
        arrived_c(zz, 1 - side)

    def load_q():
        for c in q_loads:
            c.wait()

    if groups == 4:
        z1, z2, z3 = (arrival(i) for i in range(1, groups))
        arrived_d(z1)
        swap_w(1)
        arrived_c(z, 1 - side)
        load_q()
        attend(z, 0, True)
        arrived_d(z2)
        swap_w(1)
        attend(z, 1, True)
        arrived_x(z1)
        arrived_d(z3)
        swap_w(1)
        arrived_group(z1)
        attend(z1, 0, False)
        attend(z1, 1, False)
        arrived_x(z2)
        arrived_group(z2)
        attend(z2, 0, False)
        attend(z2, 1, False)
        arrived_x(z3)
        swap_w(W_PARTS)
        arrived_group(z3)
        attend(z3, 0, False)
        swap_0 = finish(0)
        attend(z3, 1, False)
        swap_1 = finish(1)
    else:
        for i in range(1, groups):
            arrived_d(arrival(i))
        for i in range(1, groups):
            arrived_x(arrival(i))
        swap_w(W_PARTS)
        arrived_c(z, 1 - side)
        load_q()
        attend(z, 0, True)
        attend(z, 1, True)

        def step(i, carry):
            zz = arrival(i)
            arrived_group(zz)
            attend(zz, 0, False)
            attend(zz, 1, False)
            return carry

        lax.fori_loop(1, groups, step, 0)
        swap_0 = finish(0)
        swap_1 = finish(1)

    for c in w_loads:
        c.wait()
    for c in w_sends:
        c.wait_recv()

    def project(s, n):
        at = pl.ds(n * CHUNK, CHUNK)
        return (
            jnp.dot(att[0, s], wb[0, :, at], preferred_element_type=jnp.float32)
            + jnp.dot(att[1, s], wb[1, :, at], preferred_element_type=jnp.float32)
        ).astype(jnp.bfloat16)

    def place(ref, c, n):
        return ref.at[:, pl.ds(pl.multiple_of(c * half_cols + n * CHUNK, CHUNK), CHUNK)]

    swap_0.wait_recv()
    far_in = []
    for n in range(chunks):
        out = project(0, n)
        for c in range(CORES):
            far[n, c] = out[c * part : (c + 1) * part]
        for c in range(CORES):
            cc = remote(
                far.at[n, c], place(got, core, n), y_send.at[n, c], y_recv.at[n, core], y_devs[c]
            )
            cc.start()
            sent.append(cc)
            far_in.append((n, c))
    swap_1.wait_recv()
    local_copies, near_sends = [], []
    for n in range(chunks):
        out = project(1, n)
        for c in range(CORES):
            near[n, c] = out[c * part : (c + 1) * part]
        lc = pltpu.make_async_copy(near.at[n, core], place(mine, core, n), m_local.at[n])
        lc.start()
        local_copies.append(lc)
        rc = remote(near.at[n, mate], place(mine, core, n), m_send.at[n], m_recv.at[n], mate_dev)
        rc.start()
        near_sends.append(rc)

    for c in local_copies:
        c.wait()
    for n, c in enumerate(near_sends):
        c.wait_send()
        remote(
            near.at[n, mate], place(mine, mate, n), m_send.at[n], m_recv.at[n], mate_dev
        ).wait_recv()
    for c in sent:
        c.wait_send()
    for when, c in sent_if:
        pl.when(when)(c.wait_send)
    for n, c in far_in:
        remote(
            far.at[n, c], place(got, c, n), y_send.at[n, c], y_recv.at[n, c], y_devs[c]
        ).wait_recv()


def shards(groups, queries, keys, values, positions, out_weight):
    tok, width = queries.shape
    heads = width // HEAD
    run = tok // 2
    part = run // CORES
    depth, cols = out_weight.shape
    half_cols = cols // CORES
    chunks = half_cols // CHUNK
    rows = heads * run
    dma = pltpu.SemaphoreType.DMA
    out = pltpu.VMEM((part, cols), jnp.bfloat16)
    any_spec = pl.BlockSpec(memory_space=pl.ANY)
    got, mine = pl.pallas_call(
        functools.partial(kernel, groups),
        out_shape=(out, out),
        in_specs=[pl.BlockSpec(memory_space=pltpu.SMEM)] + [any_spec] * 4,
        out_specs=(pl.BlockSpec(memory_space=pltpu.VMEM),) * 2,
        scratch_shapes=[
            pltpu.VMEM((2, rows, HEAD), jnp.bfloat16),
            pltpu.VMEM((2, groups, PAIR * tok, HEAD), jnp.bfloat16),
            pltpu.VMEM((2, depth, half_cols), jnp.bfloat16),
            pltpu.VMEM((2, 2, run, width), jnp.bfloat16),
            pltpu.VMEM((2, rows, 1), jnp.float32),
            pltpu.VMEM((2, rows, 1), jnp.float32),
            pltpu.VMEM((2, rows, HEAD), jnp.float32),
            pltpu.VMEM((chunks, CORES, part, CHUNK), jnp.bfloat16),
            pltpu.VMEM((chunks, CORES, part, CHUNK), jnp.bfloat16),
            dma((2 + 2 * heads,)),
            dma((W_PARTS,)),
            dma((groups, PIECES)),
            dma((PIECES,)),
            dma((groups, PIECES)),
            dma((groups, PIECES)),
            dma((groups, PIECES)),
            dma((groups, PAIR, PIECES)),
            dma((groups, PAIR, PIECES)),
            dma((W_PARTS,)),
            dma((W_PARTS,)),
            dma((2,)),
            dma((2,)),
            dma((chunks, CORES)),
            dma((chunks, CORES)),
            dma((chunks,)),
            dma((chunks,)),
            dma((chunks,)),
        ],
        compiler_params=pltpu.CompilerParams(collective_id=0, has_side_effects=True),
    )(positions, queries, keys, values, out_weight)
    return (got.astype(jnp.float32) + mine.astype(jnp.float32)).astype(jnp.bfloat16)


def solution(mesh):
    groups = mesh.shape["cp"] // PAIR
    in_specs = (P("cp", "tp"), P("cp", None), P("cp", None), P(), P("tp", None))
    out_specs = P(("cp", "tp"), None)
    return jax.shard_map(
        functools.partial(shards, groups),
        mesh=mesh,
        in_specs=in_specs,
        out_specs=out_specs,
        check_vma=False,
    )
```

```python
import functools
import math

import jax
import jax.numpy as jnp
from jax import lax
from jax.experimental import pallas as pl
from jax.experimental.pallas import tpu as pltpu
from jax.sharding import PartitionSpec as P

HEAD = 128
GROUP = 8
CORES = 2
PAIR = 2
CHUNK = 512
W_PARTS = 8
LOG2E = math.log2(math.e)
NT = (((1,), (1,)), ((), ()))


def kernel(
    groups,
    pos_in,
    q,
    k,
    v,
    w,
    got,
    mine,
    pos,
    pos_sem,
    qs,
    kv,
    wb,
    att,
    top,
    total,
    acc,
    far,
    near,
    load_sem,
    wl_sem,
    d_send,
    d_recv,
    x_send,
    x_recv,
    c_send,
    c_recv,
    w_send,
    w_recv,
    a_send,
    a_recv,
    y_send,
    y_recv,
    m_send,
    m_recv,
    m_local,
):
    tok = q.shape[0]
    heads = q.shape[1] // HEAD
    run = tok // 2
    part = run // CORES
    half_cols = w.shape[1] // CORES
    chunks = half_cols // CHUNK
    rows = heads * run
    span = PAIR * tok

    cp = lax.axis_index("cp")
    tp = lax.axis_index("tp")
    y = tp // CORES
    core = lax.rem(tp, CORES)
    mate = 1 - core
    far_y = 1 - y
    z = cp // PAIR
    side = lax.rem(cp, PAIR)
    kv_group = tp * heads // GROUP

    def dev(c, t):
        return {"cp": c, "tp": t}

    x_dev = dev(z * PAIR + 1 - side, tp)
    mate_dev = dev(cp, y * CORES + mate)

    def remote(src, dst, ssem, rsem, to):
        return pltpu.make_async_remote_copy(
            src_ref=src,
            dst_ref=dst,
            send_sem=ssem,
            recv_sem=rsem,
            device_id=to,
            device_id_type=pl.DeviceIdType.MESH,
        )

    def block(kind, zz, ss):
        return kv.at[kind, zz, pl.ds(pl.multiple_of(ss * tok, tok), tok)]

    cols = pl.ds(pl.multiple_of(kv_group * HEAD, HEAD), HEAD)
    loads = [
        pltpu.make_async_copy(k.at[:, cols], block(0, z, side), load_sem.at[0]),
        pltpu.make_async_copy(v.at[:, cols], block(1, z, side), load_sem.at[1]),
    ]
    q_loads = []
    for s, yy in ((0, far_y), (1, y)):
        for h in range(heads):
            q_loads.append(
                pltpu.make_async_copy(
                    q.at[pl.ds(pl.multiple_of(yy * run, run), run), pl.ds(h * HEAD, HEAD)],
                    qs.at[s, pl.ds(h * run, run)],
                    load_sem.at[2 + s * heads + h],
                )
            )
    piece = half_cols // W_PARTS
    w_loads, w_sends = [], []
    for i in range(W_PARTS):
        own = pl.ds(pl.multiple_of(core * half_cols + i * piece, piece), piece)
        other = pl.ds(pl.multiple_of(mate * half_cols + i * piece, piece), piece)
        here = pl.ds(i * piece, piece)
        w_loads.append(pltpu.make_async_copy(w.at[:, own], wb.at[0, :, here], wl_sem.at[i]))
        w_sends.append(
            remote(w.at[:, other], wb.at[1, :, here], w_send.at[i], w_recv.at[i], mate_dev)
        )
    pos_load = pltpu.make_async_copy(pos_in, pos, pos_sem)
    for c in loads + q_loads + [pos_load]:
        c.start()

    barrier = pltpu.get_barrier_semaphore()
    peers = [dev(lax.rem(z + off, groups) * PAIR + side, tp) for off in range(groups - 1, 0, -1)]
    y_devs = [dev(cp, far_y * CORES + c) for c in range(CORES)]
    greet = peers + [x_dev, mate_dev] + y_devs
    for d in greet:
        pl.semaphore_signal(barrier, inc=1, device_id=d, device_id_type=pl.DeviceIdType.MESH)
    pl.semaphore_wait(barrier, len(greet))

    for c in loads:
        c.wait()
    own = block(core, z, side)
    sent = []
    x_own = remote(own, own, x_send.at[z], x_recv.at[z], x_dev)
    x_own.start()
    sent.append(x_own)
    for i, d in enumerate(peers):
        c = remote(own, own, d_send.at[i], d_recv.at[z], d)
        c.start()
        sent.append(c)
    waiting = list(w_sends)

    def swap_w(count):
        for c in waiting[:count]:
            c.start()
            sent.append(c)
        del waiting[:count]

    swap_w(3)
    for c in w_loads:
        c.start()

    def hand(kind, zz, ss):
        b = block(kind, zz, ss)
        c = remote(b, b, c_send.at[zz, ss], c_recv.at[zz, ss], mate_dev)
        c.start()
        sent.append(c)

    def arrived_x(zz):
        b = block(core, zz, 1 - side)
        remote(b, b, x_send.at[zz], x_recv.at[zz], x_dev).wait_recv()
        hand(core, zz, 1 - side)

    def arrived_d(zz):
        b = block(core, zz, side)
        remote(b, b, d_send.at[0], d_recv.at[zz], x_dev).wait_recv()
        c = remote(b, b, x_send.at[zz], x_recv.at[zz], x_dev)
        c.start()
        sent.append(c)
        hand(core, zz, side)

    def arrived_c(zz, ss):
        b = block(mate, zz, ss)
        remote(b, b, c_send.at[zz, ss], c_recv.at[zz, ss], mate_dev).wait_recv()

    def attend(zz, s, first):
        yy = far_y if s == 0 else y
        keys = kv[0, zz]
        vals = kv[1, zz]
        scores = lax.dot_general(qs[s], keys, NT, preferred_element_type=jnp.float32)
        j = lax.broadcasted_iota(jnp.int32, (1, span), 1)
        base = zz * span
        key_pos = j + pos[base]
        for i in range(1, span // run):
            key_pos = jnp.where(j >= i * run, j + (pos[base + i * run] - i * run), key_pos)
        i = lax.rem(lax.broadcasted_iota(jnp.int32, (rows, 1), 0), run)
        query_pos = i + pos[cp * tok + yy * run]
        scores = jnp.where(key_pos <= query_pos, scores, -1e30)
        peak = jnp.max(scores, axis=1, keepdims=True)
        if not first:
            old = top[s]
            peak = jnp.maximum(old, peak)
        factor = HEAD**-0.5 * LOG2E
        weights = jnp.exp2((scores - peak) * factor)
        part_sum = jnp.sum(weights, axis=1, keepdims=True)
        part_out = jnp.dot(
            weights.astype(jnp.bfloat16), vals, preferred_element_type=jnp.float32
        )
        if not first:
            fade = jnp.exp2((old - peak) * factor)
            part_sum = total[s] * fade + part_sum
            part_out = acc[s] * fade + part_out
        top[s] = peak
        total[s] = part_sum
        acc[s] = part_out

    order = [lax.rem(z + groups - off, groups) for off in range(groups - 1, 0, -1)]
    arrived_x(z)
    small = groups <= 4
    for c in q_loads + [pos_load]:
        c.wait()

    def finish(s):
        out = (acc[s] / total[s]).astype(jnp.bfloat16)
        for h in range(heads):
            att[0, s, :, h * HEAD : (h + 1) * HEAD] = out[h * run : (h + 1) * run]
        c = remote(att.at[0, s], att.at[1, s], a_send.at[s], a_recv.at[s], mate_dev)
        c.start()
        sent.append(c)
        return c

    def own_group():
        arrived_c(z, 1 - side)
        attend(z, 0, True)
        attend(z, 1, True)

    if small:
        z1, z2, z3 = order
        arrived_d(z1)
        swap_w(1)
        arrived_c(z, 1 - side)
        attend(z, 0, True)
        arrived_d(z2)
        swap_w(1)
        attend(z, 1, True)
        arrived_d(z3)
        arrived_x(z1)
        swap_w(1)
        arrived_c(z1, side)
        arrived_c(z1, 1 - side)
        attend(z1, 0, False)
        arrived_x(z2)
        attend(z1, 1, False)
        arrived_x(z3)
        swap_w(W_PARTS)
        arrived_c(z2, side)
        arrived_c(z2, 1 - side)
        attend(z2, 0, False)
        arrived_c(z3, side)
        arrived_c(z3, 1 - side)
        attend(z3, 0, False)
        swap_0 = finish(0)
        attend(z2, 1, False)
        attend(z3, 1, False)
        swap_1 = finish(1)
    else:
        for zz in order:
            arrived_d(zz)
        for zz in order:
            arrived_x(zz)
        swap_w(W_PARTS)
        own_group()

        def step(off, carry):
            zz = lax.rem(z + groups - off, groups)
            arrived_c(zz, side)
            arrived_c(zz, 1 - side)
            attend(zz, 0, False)
            attend(zz, 1, False)
            return carry

        lax.fori_loop(1, groups, step, 0)
        swap_0 = finish(0)
        swap_1 = finish(1)

    for c in w_loads:
        c.wait()
    for c in w_sends:
        c.wait_recv()

    def project(s, n):
        at = pl.ds(n * CHUNK, CHUNK)
        return (
            jnp.dot(att[0, s], wb[0, :, at], preferred_element_type=jnp.float32)
            + jnp.dot(att[1, s], wb[1, :, at], preferred_element_type=jnp.float32)
        ).astype(jnp.bfloat16)

    def place(ref, c, n):
        return ref.at[:, pl.ds(pl.multiple_of(c * half_cols + n * CHUNK, CHUNK), CHUNK)]

    swap_0.wait_recv()
    far_in = []
    for n in range(chunks):
        out = project(0, n)
        for c in range(CORES):
            far[n, c] = out[c * part : (c + 1) * part]
        for c in range(CORES):
            cc = remote(
                far.at[n, c], place(got, core, n), y_send.at[n, c], y_recv.at[n, core], y_devs[c]
            )
            cc.start()
            sent.append(cc)
            far_in.append((n, c))
    swap_1.wait_recv()
    local_copies, near_sends = [], []
    for n in range(chunks):
        out = project(1, n)
        for c in range(CORES):
            near[n, c] = out[c * part : (c + 1) * part]
        lc = pltpu.make_async_copy(near.at[n, core], place(mine, core, n), m_local.at[n])
        lc.start()
        local_copies.append(lc)
        rc = remote(near.at[n, mate], place(mine, core, n), m_send.at[n], m_recv.at[n], mate_dev)
        rc.start()
        near_sends.append(rc)

    for c in local_copies:
        c.wait()
    for n, c in enumerate(near_sends):
        c.wait_send()
        remote(
            near.at[n, mate], place(mine, mate, n), m_send.at[n], m_recv.at[n], mate_dev
        ).wait_recv()
    for c in sent:
        c.wait_send()
    for n, c in far_in:
        remote(
            far.at[n, c], place(got, c, n), y_send.at[n, c], y_recv.at[n, c], y_devs[c]
        ).wait_recv()


def shards(groups, queries, keys, values, positions, out_weight):
    tok, width = queries.shape
    heads = width // HEAD
    run = tok // 2
    part = run // CORES
    depth, cols = out_weight.shape
    half_cols = cols // CORES
    chunks = half_cols // CHUNK
    rows = heads * run
    dma = pltpu.SemaphoreType.DMA
    out = pltpu.VMEM((part, cols), jnp.bfloat16)
    any_spec = pl.BlockSpec(memory_space=pl.ANY)
    got, mine = pl.pallas_call(
        functools.partial(kernel, groups),
        out_shape=(out, out),
        in_specs=[any_spec] * 5,
        out_specs=(pl.BlockSpec(memory_space=pltpu.VMEM),) * 2,
        scratch_shapes=[
            pltpu.SMEM(positions.shape, jnp.int32),
            dma(()),
            pltpu.VMEM((2, rows, HEAD), jnp.bfloat16),
            pltpu.VMEM((2, groups, PAIR * tok, HEAD), jnp.bfloat16),
            pltpu.VMEM((2, depth, half_cols), jnp.bfloat16),
            pltpu.VMEM((2, 2, run, width), jnp.bfloat16),
            pltpu.VMEM((2, rows, 1), jnp.float32),
            pltpu.VMEM((2, rows, 1), jnp.float32),
            pltpu.VMEM((2, rows, HEAD), jnp.float32),
            pltpu.VMEM((chunks, CORES, part, CHUNK), jnp.bfloat16),
            pltpu.VMEM((chunks, CORES, part, CHUNK), jnp.bfloat16),
            dma((2 + 2 * heads,)),
            dma((W_PARTS,)),
            dma((groups,)),
            dma((groups,)),
            dma((groups,)),
            dma((groups,)),
            dma((groups, PAIR)),
            dma((groups, PAIR)),
            dma((W_PARTS,)),
            dma((W_PARTS,)),
            dma((2,)),
            dma((2,)),
            dma((chunks, CORES)),
            dma((chunks, CORES)),
            dma((chunks,)),
            dma((chunks,)),
            dma((chunks,)),
        ],
        compiler_params=pltpu.CompilerParams(collective_id=0, has_side_effects=True),
    )(positions, queries, keys, values, out_weight)
    return (got.astype(jnp.float32) + mine.astype(jnp.float32)).astype(jnp.bfloat16)


def solution(mesh):
    groups = mesh.shape["cp"] // PAIR
    in_specs = (P("cp", "tp"), P("cp", None), P("cp", None), P(), P("tp", None))
    out_specs = P(("cp", "tp"), None)
    return jax.shard_map(
        functools.partial(shards, groups),
        mesh=mesh,
        in_specs=in_specs,
        out_specs=out_specs,
        check_vma=False,
    )
```
